32 devices in a mesh: samp: 16 (over z, y, x), feat: 2 (over core).
Axes of the slice: x: 2, y: 2, z: 4, core: 2. Of those that a mesh axis runs over, the one named last changes fastest.
Arguments:
- design_matrix: bfloat16 [2048, 32768], P('samp', 'feat'), may hold values from -0.046875 to 0.046875
- labels: int32 [2048], P('samp'), may hold values from 0 to 1
- weights: float32 [16, 32768], P(None, ('feat', 'samp')), may hold values from -6 to 6
- lambdas: float32 [16], replicated, may hold values from 0.05 to 1
- sketch: bfloat16 [32768, 384], P(('feat', 'samp')), may hold values from -0.03125 to 0.03125
- sketch_values: float32 [384], replicated, may hold values from 0.05 to 2
Outputs:
- new_weights: float32 [16, 32768], P(None, ('feat', 'samp'))
The draws below stay inside these ranges and needn't reach their ends.
All inputs are finite; a program needn't handle non-finite values.
Results may differ from the reference program's by a relative error of at most 0.004.
Values may be sent and summed in bfloat16 or wider, within the bound.
A program may use at most 64 MiB of HBM per device.

```python
import math
import jax
import jax.numpy as jnp
from jax import lax

FEATURES = 32768
RANK = 384
STRENGTHS = 16
ITERS = 2
SAMPLES = 2048


def place_ends(result, key, low, largest):
    shape = result.shape
    index_at = [jax.random.randint(jax.random.fold_in(key, axis), (), 0, shape[axis]) for axis in range(len(shape))]
    result = result.at[tuple(index_at)].set(low)
    longest = shape.index(max(shape))
    index_at[longest] = (index_at[longest] + 1) % shape[longest]
    return result.at[tuple(index_at)].set(largest)


def strengthened(array, own_key, source, target, blocks, factor):
    owner, partner = [(jnp.arange(array.shape[position]) // (array.shape[position] // blocks)).reshape([-1 if axis == position else 1 for axis in range(array.ndim)]) for position in (source, target)]
    chosen = jax.random.permutation(own_key, blocks)[partner]
    strong = (owner == chosen) | (owner == (partner + blocks // 2) % blocks)
    return jnp.where(strong, factor * array, array)


def shard_levels(own_key, shape, pieces, low, top_value):
    gain, own = 1.0, jax.random.fold_in(own_key, 6)
    for position, shards_of in pieces:
        steps = jnp.exp(jax.random.uniform(jax.random.fold_in(own, position), (shards_of,), jnp.float32, low / len(pieces), top_value / len(pieces)))
        gain = gain * jnp.repeat(steps, shape[position] // shards_of).reshape([-1 if axis == position else 1 for axis in range(len(shape))])
    return gain


def noise(stream_key, extent, width, most, split=(), held_as=jnp.bfloat16):
    gain = shard_levels(stream_key, extent, split, -0.22, 0.18) if split else 1.0
    values = jax.random.normal(stream_key, extent, jnp.float32) * width * gain
    return jnp.minimum(jnp.maximum(values, -most), most).astype(held_as)


def heavy_noise(key, shape, scale, bound, shards, heavy, kind=jnp.bfloat16):
    values = scale * jax.random.normal(key, shape, jnp.float32)
    if shards:
        values = values * shard_levels(key, shape, shards, -0.22, 0.18)
    return jnp.clip(strengthened(values, jax.random.fold_in(key, 3), *heavy), -bound, bound).astype(kind)


def setup_inputs(seed: int = 0) -> dict:
    arg_keys = jax.random.split(jax.random.key(seed), 7)
    design_matrix = heavy_noise(arg_keys[0], (SAMPLES, FEATURES), FEATURES ** -0.5, 0.046875, ((0, 16), (1, 2)), (0, 1, 16, 2.0))
    labels = place_ends(jax.random.randint(arg_keys[1], (SAMPLES,), 0, 2), jax.random.fold_in(arg_keys[1], 1), 0, 1).astype(jnp.int32)
    weights = noise(arg_keys[2], (STRENGTHS, FEATURES), 1.0, 6.0, ((1, 32),), jnp.float32)
    lambdas = jnp.clip(jnp.exp(jax.random.uniform(arg_keys[3], (STRENGTHS,), jnp.float32, math.log(0.05), math.log(1.0))), 0.05, 1.0)
    sketch = noise(arg_keys[4], (FEATURES, RANK), FEATURES ** -0.5, 0.03125, ((0, 32),))
    sketch_values = jnp.clip(jnp.exp(jax.random.uniform(arg_keys[5], (RANK,), jnp.float32, math.log(0.05), math.log(2.0))), 0.05, 2.0)
    return dict(design_matrix=design_matrix, labels=labels, weights=weights, lambdas=lambdas, sketch=sketch, sketch_values=sketch_values)


def reference(design_matrix, labels, weights, lambdas, sketch, sketch_values):
    sketch_full = sketch.astype(jnp.float32)
    smallest = jnp.min(sketch_values)
    ratios = (smallest + lambdas[:, None]) / (sketch_values[None, :] + lambdas[:, None]) - 1.0

    def apply_rows(vector):
        return lax.dot_general(vector.astype(jnp.bfloat16), design_matrix, (((1,), (1,)), ((), ())), preferred_element_type=jnp.float32)

    def apply_columns(values):
        return jnp.dot(values, design_matrix, preferred_element_type=jnp.float32)

    def precondition(residual):
        projected = jnp.dot(residual, sketch_full, precision=lax.Precision.HIGHEST)
        correction = lax.dot_general(ratios * projected, sketch_full, (((1,), (1,)), ((), ())), precision=lax.Precision.HIGHEST)
        precond_res = residual + correction
        return precond_res, jnp.sum(residual * precond_res, axis=1)

    logits = apply_rows(weights)
    probability = jax.nn.sigmoid(logits)
    hessian_diag = probability * (1.0 - probability)
    miss_rows = (probability - labels[None, :].astype(jnp.float32)).astype(jnp.bfloat16)
    gradient = apply_columns(miss_rows) + lambdas[:, None] * weights
    residual = -gradient
    precond_res, res_dot = precondition(residual)
    direction = precond_res
    update = jnp.zeros_like(weights)
    for iteration in range(ITERS):
        image_rows = apply_rows(direction)
        hess_dir = apply_columns((hessian_diag * image_rows).astype(jnp.bfloat16)) + lambdas[:, None] * direction
        step_size = res_dot / jnp.sum(direction * hess_dir, axis=1)
        update = update + step_size[:, None] * direction
        if iteration + 1 < ITERS:
            residual = residual - step_size[:, None] * hess_dir
            precond_res, new_dot = precondition(residual)
            direction = precond_res + (new_dot / res_dot)[:, None] * direction
            res_dot = new_dot
    return weights + update
```

```python
import functools

import jax
import jax.numpy as jnp
from jax import lax
from jax.experimental import pallas as pl
from jax.experimental.pallas import tpu as pltpu
from jax.sharding import PartitionSpec as P

ITERS = 2


def shards(design_matrix, labels, weights, lambdas, sketch, sketch_values):
    sketch_full = sketch.astype(jnp.float32)
    smallest = jnp.min(sketch_values)
    ratios = (smallest + lambdas[:, None]) / (sketch_values[None, :] + lambdas[:, None]) - 1.0

    def apply_rows(vector):
        vector_half = vector.astype(jnp.bfloat16)
        partial_rows = lax.dot_general(
            lax.all_gather(vector_half, "samp", axis=1, tiled=True),
            design_matrix,
            (((1,), (1,)), ((), ())),
            preferred_element_type=jnp.float32,
        )
        return lax.psum(partial_rows, "feat")

    def apply_columns(values):
        return lax.psum_scatter(
            lax.dot_general(
                design_matrix, values, (((0,), (1,)), ((), ())), preferred_element_type=jnp.float32
            ),
            "samp",
            scatter_dimension=0,
            tiled=True,
        ).T

    def precondition(residual):
        projected = jnp.dot(residual, sketch_full, precision=lax.Precision.HIGHEST)
        projected = lax.psum(projected, ("samp", "feat"))
        correction = lax.dot_general(
            ratios * projected,
            sketch_full,
            (((1,), (1,)), ((), ())),
            precision=lax.Precision.HIGHEST,
        )
        precond_res = residual + correction
        res_dot = lax.psum(jnp.sum(residual * precond_res, axis=1), ("samp", "feat"))
        return (precond_res, res_dot)

    logits = apply_rows(weights)
    probability = jax.nn.sigmoid(logits)
    hessian_diag = probability * (1.0 - probability)
    miss_rows = (probability - labels[None, :].astype(jnp.float32)).astype(jnp.bfloat16)
    gradient = apply_columns(miss_rows) + lambdas[:, None] * weights
    residual = -gradient
    precond_res, res_dot = precondition(residual)
    direction = precond_res
    update = jnp.zeros_like(residual)
    for iteration in range(ITERS):
        image_rows = apply_rows(direction)
        hess_dir = (
            apply_columns((hessian_diag * image_rows).astype(jnp.bfloat16))
            + lambdas[:, None] * direction
        )
        curvature = lax.psum(jnp.sum(direction * hess_dir, axis=1), ("samp", "feat"))
        step_size = res_dot / curvature
        update = update + step_size[:, None] * direction
        if iteration + 1 < ITERS:
            residual = residual - step_size[:, None] * hess_dir
            precond_res, new_dot = precondition(residual)
            direction = precond_res + (new_dot / res_dot)[:, None] * direction
            res_dot = new_dot
    return weights + update


MESH = pl.DeviceIdType.MESH
LANES = 128
PLANE = 4


def lane_sums(values):
    total = values[:, :LANES]
    for start in range(LANES, values.shape[1], LANES):
        total = total + values[:, start : start + LANES]
    return total


def split(values):
    high = values.astype(jnp.bfloat16)
    low = (values - high.astype(jnp.float32)).astype(jnp.bfloat16)
    return jnp.concatenate([high, low], axis=0)


def kernel(
    n, feats, design_hbm, labels, weights, lambdas, sketch_hbm, sketch_values, out,
    design, sketch, gathered, summed, arrived, rows_mine, rows_theirs,
    proj_mine, proj_theirs, proj_full, plane_mine, plane_theirs, line_mine, line_theirs,
    curve, design_sem, sketch_sem, gather_sems, sum_sems, row_sems, proj_sems,
    plane_sems, line_sems, back_sems, curve_sems,
):
    me = lax.axis_index("samp")
    side = lax.axis_index("feat")
    strengths, width = weights.shape
    rank = sketch.shape[1]
    band = strengths // feats
    planes = n // PLANE

    def fetch(chunk):
        return pltpu.make_async_copy(
            design_hbm.at[:, pl.ds(chunk * width, width)], design.at[chunk], design_sem.at[chunk]
        )

    for chunk in range(n):
        fetch(chunk).start()
    sketch_copy = pltpu.make_async_copy(sketch_hbm, sketch, sketch_sem)
    sketch_copy.start()

    def put(source, target, sems, slot, samp, feat):
        return pltpu.make_async_remote_copy(
            src_ref=source, dst_ref=target,
            send_sem=sems.at[(0, *slot)], recv_sem=sems.at[(1, *slot)],
            device_id=(samp, feat), device_id_type=MESH,
        )

    barrier = pltpu.get_barrier_semaphore()
    for step in range(1, n):
        pl.semaphore_signal(
            barrier, inc=1, device_id=(lax.rem(me + step, n), side), device_id_type=MESH
        )
    for step in range(1, feats):
        pl.semaphore_signal(
            barrier, inc=1, device_id=(me, lax.rem(side + step, feats)), device_id_type=MESH
        )
    gathered[0, me] = weights[...].astype(jnp.bfloat16)
    pl.semaphore_wait(barrier, n - 1 + feats - 1)

    def ahead(step):
        return lax.rem(me + step, n)

    def behind(step):
        return lax.rem(me + n - step, n)

    def apply_rows(phase):
        def copy(step):
            own = gathered.at[phase, me]
            return put(own, own, gather_sems, (phase, step), ahead(step), side)

        def multiply(chunk, carry):
            rows, squares = carry
            if phase == 0:
                fetch(chunk).wait()
            block = gathered[phase, chunk]
            rows = rows + lax.dot_general(
                block, design[chunk], (((1,), (1,)), ((), ())), preferred_element_type=jnp.float32
            )
            if phase > 0:
                block = block.astype(jnp.float32)
                squares = squares + lane_sums(block * block)
            return rows, squares

        for step in range(1, n):
            copy(step).start()
        zero = jnp.zeros((strengths, LANES), jnp.float32)
        carry = (jnp.zeros((strengths, design.shape[1]), jnp.float32), zero)
        carry = multiply(me, carry)

        def body(step, carry):
            copy(step).wait_recv()
            return multiply(behind(step), carry)

        rows, squares = lax.fori_loop(1, n, body, carry)
        rows_mine[phase, 0] = rows
        rows_mine[phase, 1] = squares

        def swap(step):
            return put(
                rows_mine.at[phase], rows_theirs.at[phase, step], row_sems, (phase, step),
                me, lax.rem(side + step, feats),
            )

        for step in range(1, feats):
            swap(step).start()
        for step in range(1, feats):
            swap(step).wait()
            rows = rows + rows_theirs[phase, step, 0]
            squares = squares + rows_theirs[phase, step, 1]
        for step in range(1, n):
            copy(step).wait_send()
        return rows, jnp.sum(squares, axis=1, keepdims=True)

    def apply_columns(phase, values):
        def copy(step):
            return put(
                summed.at[phase, step], arrived.at[phase, step], sum_sems, (phase, step),
                ahead(step), side,
            )

        def multiply(chunk):
            return jnp.dot(values, design[chunk], preferred_element_type=jnp.float32)

        def send(step, _):
            summed[phase, step] = multiply(ahead(step)).astype(summed.dtype)
            copy(step).start()
            return 0

        lax.fori_loop(1, n, send, 0)

        def take(step, total):
            copy(step).wait()
            return total + arrived[phase, step].astype(jnp.float32)

        return lax.fori_loop(1, n, take, multiply(me))

    def project(phase, residual):
        if phase == 0:
            sketch_copy.wait()
        parts = jnp.dot(split(residual), sketch[...], preferred_element_type=jnp.float32)
        total = jnp.concatenate(
            [parts[:strengths] + parts[strengths:], lane_sums(residual * residual)], axis=1
        )
        for step in range(feats):
            proj_mine[phase, step] = total[step * band : (step + 1) * band]

        def swap(step):
            other = lax.rem(side + step, feats)
            return put(
                proj_mine.at[phase, other], proj_theirs.at[phase, step], proj_sems,
                (phase, step), me, other,
            )

        for step in range(1, feats):
            swap(step).start()
        part = proj_mine[phase, side]
        for step in range(1, feats):
            swap(step).wait()
            part = part + proj_theirs[phase, step]

        plane_mine[phase] = part
        corner = me // PLANE * PLANE

        def across(step):
            return put(
                plane_mine.at[phase], plane_theirs.at[phase, step], plane_sems, (phase, step),
                corner + lax.rem(me - corner + step, PLANE), side,
            )

        for step in range(1, PLANE):
            across(step).start()
        for step in range(1, PLANE):
            across(step).wait()
            part = part + plane_theirs[phase, step]

        line_mine[phase] = part

        def along(step):
            return put(
                line_mine.at[phase], line_theirs.at[phase, step], line_sems, (phase, step),
                lax.rem(me + step * PLANE, n), side,
            )

        for step in range(1, planes):
            along(step).start()
        for step in range(1, planes):
            along(step).wait()
            part = part + line_theirs[phase, step]

        proj_full[phase, side] = part

        def back(step):
            return put(
                proj_full.at[phase, side], proj_full.at[phase, side], back_sems, (phase, step),
                me, lax.rem(side + step, feats),
            )

        for step in range(1, feats):
            back(step).start()
        for step in range(1, feats):
            other = lax.rem(side + feats - step, feats)
            put(
                proj_full.at[phase, other], proj_full.at[phase, other], back_sems, (phase, step),
                me, other,
            ).wait_recv()
        for step in range(1, feats):
            back(step).wait_send()
        total = jnp.concatenate([proj_full[phase, step] for step in range(feats)], axis=0)
        return total[:, :rank], jnp.sum(total[:, rank:], axis=1, keepdims=True)

    def precondition(phase, residual):
        projected, norm = project(phase, residual)
        weighted = ratios * projected
        parts = lax.dot_general(
            split(weighted), sketch[...], (((1,), (1,)), ((), ())),
            preferred_element_type=jnp.float32,
        )
        res_dot = norm + jnp.sum(weighted * projected, axis=1, keepdims=True)
        return residual + parts[:strengths] + parts[strengths:], res_dot

    diagonal = (
        lax.broadcasted_iota(jnp.int32, (strengths, LANES), 0)
        == lax.broadcasted_iota(jnp.int32, (strengths, LANES), 1)
    ).astype(jnp.float32)

    def share(phase, values):
        column = jnp.sum(values, axis=1, keepdims=True)
        curve[phase, 0] = jnp.sum(column * diagonal, axis=0, keepdims=True)

        def copy(step):
            return put(
                curve.at[phase, 0], curve.at[phase, step], curve_sems, (phase, step),
                ahead(step), side,
            )

        for step in range(1, n):
            copy(step).start()
        return copy

    def collect(phase, copy):
        for step in range(1, n):
            copy(step).wait()
        total = curve[phase, 0]
        for step in range(1, n):
            total = total + curve[phase, step]
        return jnp.sum(total * diagonal, axis=1, keepdims=True)

    strength = lambdas[...]
    spectrum = sketch_values[...]
    smallest = jnp.min(spectrum, axis=1, keepdims=True)
    ratios = (smallest + strength) / (spectrum + strength) - 1.0

    logits, _ = apply_rows(0)
    probability = jax.nn.sigmoid(logits)
    hessian_diag = probability * (1.0 - probability)
    miss_rows = (probability - labels[...].astype(jnp.float32)).astype(jnp.bfloat16)
    residual = -(apply_columns(0, miss_rows) + strength * weights[...])
    direction, res_dot = precondition(0, residual)
    update = jnp.zeros_like(residual)
    for iteration in range(ITERS):
        gathered[iteration + 1, me] = direction.astype(jnp.bfloat16)
        image, squares = apply_rows(iteration + 1)
        bent = (hessian_diag * image).astype(jnp.bfloat16)
        copy = share(iteration, bent.astype(jnp.float32) * image)
        last = iteration + 1 == ITERS
        if not last:
            hess_dir = apply_columns(iteration + 1, bent) + strength * direction
        curvature = collect(iteration, copy) + strength * squares
        step_size = res_dot / curvature
        update = update + step_size * direction
        if not last:
            residual = residual - step_size * hess_dir
            precond_res, new_dot = precondition(iteration + 1, residual)
            direction = precond_res + (new_dot / res_dot) * direction
            res_dot = new_dot
    out[...] = weights[...] + update


def fused(n, feats, design_matrix, labels, weights, lambdas, sketch, sketch_values):
    strengths, width = weights.shape
    samples = design_matrix.shape[0]
    rank = sketch.shape[1]
    band = (strengths // feats, rank + LANES)
    dma = pltpu.SemaphoreType.DMA
    f32, bf16 = jnp.float32, jnp.bfloat16
    vmem = pl.BlockSpec(memory_space=pltpu.VMEM)
    anywhere = pl.BlockSpec(memory_space=pl.ANY)
    return pl.pallas_call(
        functools.partial(kernel, n, feats),
        out_shape=jax.ShapeDtypeStruct(weights.shape, f32),
        in_specs=[anywhere, vmem, vmem, vmem, anywhere, vmem],
        out_specs=vmem,
        scratch_shapes=[
            pltpu.VMEM((n, samples, width), bf16),
            pltpu.VMEM(sketch.shape, bf16),
            pltpu.VMEM((ITERS + 1, n, strengths, width), bf16),
            pltpu.VMEM((ITERS, n, strengths, width), bf16),
            pltpu.VMEM((ITERS, n, strengths, width), bf16),
            pltpu.VMEM((ITERS + 1, 2, strengths, samples), f32),
            pltpu.VMEM((ITERS + 1, feats, 2, strengths, samples), f32),
            pltpu.VMEM((ITERS, feats, *band), f32),
            pltpu.VMEM((ITERS, feats, *band), f32),
            pltpu.VMEM((ITERS, feats, *band), f32),
            pltpu.VMEM((ITERS, *band), f32),
            pltpu.VMEM((ITERS, PLANE, *band), f32),
            pltpu.VMEM((ITERS, *band), f32),
            pltpu.VMEM((ITERS, n // PLANE, *band), f32),
            pltpu.VMEM((ITERS, n, 1, LANES), f32),
            dma((n,)),
            dma,
            dma((2, ITERS + 1, n)),
            dma((2, ITERS, n)),
            dma((2, ITERS + 1, feats)),
            dma((2, ITERS, feats)),
            dma((2, ITERS, PLANE)),
            dma((2, ITERS, n // PLANE)),
            dma((2, ITERS, feats)),
            dma((2, ITERS, n)),
        ],
        compiler_params=pltpu.CompilerParams(
            collective_id=0, has_side_effects=True, vmem_limit_bytes=48 * 1024 * 1024
        ),
    )(
        design_matrix, labels[None, :], weights, lambdas[:, None], sketch, sketch_values[None, :]
    )


def solution(mesh):
    n, feats = mesh.shape["samp"], mesh.shape["feat"]

    def local(design_matrix, labels, weights, lambdas, sketch, sketch_values):
        strengths, width = weights.shape
        whole = (
            width % LANES == 0
            and design_matrix.shape[0] == LANES
            and sketch.shape[1] % LANES == 0
            and n % PLANE == 0
            and strengths % (8 * feats) == 0
            and strengths <= LANES
        )
        run = functools.partial(fused, n, feats) if whole else shards
        return run(design_matrix, labels, weights, lambdas, sketch, sketch_values)

    return jax.shard_map(
        local,
        mesh=mesh,
        in_specs=(
            P("samp", "feat"),
            P("samp"),
            P(None, ("feat", "samp")),
            P(),
            P(("feat", "samp"), None),
            P(),
        ),
        out_specs=P(None, ("feat", "samp")),
        check_vma=False,
    )
```

```python
import functools

import jax
import jax.numpy as jnp
from jax import lax
from jax.experimental import pallas as pl
from jax.experimental.pallas import tpu as pltpu
from jax.sharding import PartitionSpec as P

ITERS = 2


def shards(design_matrix, labels, weights, lambdas, sketch, sketch_values):
    sketch_full = sketch.astype(jnp.float32)
    smallest = jnp.min(sketch_values)
    ratios = (smallest + lambdas[:, None]) / (sketch_values[None, :] + lambdas[:, None]) - 1.0

    def apply_rows(vector):
        vector_half = vector.astype(jnp.bfloat16)
        partial_rows = lax.dot_general(
            lax.all_gather(vector_half, "samp", axis=1, tiled=True),
            design_matrix,
            (((1,), (1,)), ((), ())),
            preferred_element_type=jnp.float32,
        )
        return lax.psum(partial_rows, "feat")

    def apply_columns(values):
        return lax.psum_scatter(
            lax.dot_general(
                design_matrix, values, (((0,), (1,)), ((), ())), preferred_element_type=jnp.float32
            ),
            "samp",
            scatter_dimension=0,
            tiled=True,
        ).T

    def precondition(residual):
        projected = jnp.dot(residual, sketch_full, precision=lax.Precision.HIGHEST)
        projected = lax.psum(projected, ("samp", "feat"))
        correction = lax.dot_general(
            ratios * projected,
            sketch_full,
            (((1,), (1,)), ((), ())),
            precision=lax.Precision.HIGHEST,
        )
        precond_res = residual + correction
        res_dot = lax.psum(jnp.sum(residual * precond_res, axis=1), ("samp", "feat"))
        return (precond_res, res_dot)

    logits = apply_rows(weights)
    probability = jax.nn.sigmoid(logits)
    hessian_diag = probability * (1.0 - probability)
    miss_rows = (probability - labels[None, :].astype(jnp.float32)).astype(jnp.bfloat16)
    gradient = apply_columns(miss_rows) + lambdas[:, None] * weights
    residual = -gradient
    precond_res, res_dot = precondition(residual)
    direction = precond_res
    update = jnp.zeros_like(residual)
    for iteration in range(ITERS):
        image_rows = apply_rows(direction)
        hess_dir = (
            apply_columns((hessian_diag * image_rows).astype(jnp.bfloat16))
            + lambdas[:, None] * direction
        )
        curvature = lax.psum(jnp.sum(direction * hess_dir, axis=1), ("samp", "feat"))
        step_size = res_dot / curvature
        update = update + step_size[:, None] * direction
        if iteration + 1 < ITERS:
            residual = residual - step_size[:, None] * hess_dir
            precond_res, new_dot = precondition(residual)
            direction = precond_res + (new_dot / res_dot)[:, None] * direction
            res_dot = new_dot
    return weights + update


MESH = pl.DeviceIdType.MESH
LANES = 128
PLANE = 4


def lane_sums(values):
    total = values[:, :LANES]
    for start in range(LANES, values.shape[1], LANES):
        total = total + values[:, start : start + LANES]
    return total


def split(values):
    high = values.astype(jnp.bfloat16)
    low = (values - high.astype(jnp.float32)).astype(jnp.bfloat16)
    return jnp.concatenate([high, low], axis=0)


def kernel(
    n, feats, design_hbm, labels, weights, lambdas, sketch_hbm, sketch_values, out,
    design, sketch, gathered, half_mine, half_theirs, summed, arrived, rows_mine, rows_theirs,
    proj_mine, proj_theirs, proj_full, plane_mine, plane_theirs, line_mine, line_theirs,
    curve, design_sem, sketch_sem, gather_sems, sum_sems, row_sems, proj_sems,
    plane_sems, line_sems, back_sems, curve_sems,
):
    me = lax.axis_index("samp")
    side = lax.axis_index("feat")
    strengths, width = weights.shape
    rank = sketch.shape[1]
    band = strengths // feats
    planes = n // PLANE

    def fetch(chunk):
        return pltpu.make_async_copy(
            design_hbm.at[:, pl.ds(chunk * width, width)], design.at[chunk], design_sem.at[chunk]
        )

    for chunk in range(n):
        fetch(chunk).start()
    sketch_copy = pltpu.make_async_copy(sketch_hbm, sketch, sketch_sem)
    sketch_copy.start()

    def put(source, target, sems, slot, samp, feat):
        return pltpu.make_async_remote_copy(
            src_ref=source, dst_ref=target,
            send_sem=sems.at[(0, *slot)], recv_sem=sems.at[(1, *slot)],
            device_id=(samp, feat), device_id_type=MESH,
        )

    barrier = pltpu.get_barrier_semaphore()
    for step in range(1, n):
        pl.semaphore_signal(
            barrier, inc=1, device_id=(lax.rem(me + step, n), side), device_id_type=MESH
        )
    for step in range(1, feats):
        pl.semaphore_signal(
            barrier, inc=1, device_id=(me, lax.rem(side + step, feats)), device_id_type=MESH
        )
    gathered[0, me] = weights[...].astype(jnp.bfloat16)
    pl.semaphore_wait(barrier, n - 1 + feats - 1)

    def ahead(step):
        return lax.rem(me + step, n)

    column = lax.rem(me, 2)
    line = lax.rem(me // 2, 2)
    beside = me + 1 - 2 * column
    below = me + 2 - 4 * line
    across = beside + 2 - 4 * line
    half = width // 2

    def at(place, step):
        return lax.rem(place + step * PLANE, n)

    def apply_rows(phase):
        copies = []

        def send(chunk, kind, step, target, part=slice(None)):
            block = gathered.at[phase, chunk, :, part]
            copy = put(block, block, gather_sems, (phase, kind, step), target, side)
            copy.start()
            copies.append(copy)

        def receive(chunk, kind, step, part=slice(None)):
            block = gathered.at[phase, chunk, :, part]
            put(block, block, gather_sems, (phase, kind, step), beside, side).wait_recv()

        def multiply(chunk, carry):
            rows, squares = carry
            if phase == 0:
                fetch(chunk).wait()
            block = gathered[phase, chunk]
            rows = rows + lax.dot_general(
                block, design[chunk], (((1,), (1,)), ((), ())), preferred_element_type=jnp.float32
            )
            if phase > 0:
                block = block.astype(jnp.float32)
                squares = squares + lane_sums(block * block)
            return rows, squares

        left, right = slice(0, half), slice(half, width)
        send(me, 0, 0, beside)
        send(me, 1, 0, below)
        for step in range(1, planes):
            send(me, 4, step, at(me, step))
        zero = jnp.zeros((strengths, LANES), jnp.float32)
        carry = (jnp.zeros((strengths, design.shape[1]), jnp.float32), zero)
        carry = multiply(me, carry)
        for step in range(planes):
            if step + 1 < planes:
                chunk = at(me, planes - step - 1)
                receive(chunk, 4, step + 1)
                send(chunk, 0, step + 1, beside)
                send(chunk, 1, step + 1, below)
                carry = multiply(chunk, carry)
            chunk = at(beside, planes - step)
            receive(chunk, 0, step)
            send(chunk, 2, step, below, left)
            other = at(below, planes - step)
            receive(other, 1, step)
            send(other, 3, step, beside, right)
            carry = multiply(chunk, carry)
            carry = multiply(other, carry)
        for step in range(planes):
            chunk = at(across, planes - step)
            receive(chunk, 2, step, left)
            receive(chunk, 3, step, right)
            carry = multiply(chunk, carry)
        rows, squares = carry
        rows_mine[phase, 0] = rows
        rows_mine[phase, 1] = squares

        def swap(step):
            return put(
                rows_mine.at[phase], rows_theirs.at[phase, step], row_sems, (phase, step),
                me, lax.rem(side + step, feats),
            )

        for step in range(1, feats):
            swap(step).start()
        for step in range(1, feats):
            swap(step).wait()
            rows = rows + rows_theirs[phase, step, 0]
            squares = squares + rows_theirs[phase, step, 1]
        for copy in copies:
            copy.wait_send()
        return rows, jnp.sum(squares, axis=1, keepdims=True)

    def encode(values):
        return (values * values * values).astype(jnp.bfloat16)

    def decode(values):
        values = values.astype(jnp.float32)
        root = jnp.exp(jnp.log(jnp.abs(values)) * (1.0 / 3.0))
        return jnp.where(values < 0, -root, root)

    def apply_columns(phase, values):
        def halves(kind, step, target):
            return put(
                half_mine.at[phase, kind, step], half_theirs.at[phase, kind, step], sum_sems,
                (phase, kind, step), target, side,
            )

        def blocks(kind, step, target):
            return put(
                summed.at[phase, kind, step], arrived.at[phase, kind, step], sum_sems,
                (phase, 2 + kind, step), target, side,
            )

        def multiply(chunk):
            return jnp.dot(values, design[chunk], preferred_element_type=jnp.float32)

        steps = (*range(1, planes), 0)
        for step in steps:
            part = encode(multiply(at(across, step)))
            half_mine[phase, 0, step] = part[:, :half]
            half_mine[phase, 1, step] = part[:, half:]
            halves(0, step, beside).start()
            halves(1, step, below).start()
        for step in steps:
            part = multiply(at(beside, step))
            halves(1, step, below).wait_recv()
            summed[phase, 0, step, :, :half] = encode(part[:, :half])
            summed[phase, 0, step, :, half:] = encode(
                part[:, half:] + decode(half_theirs[phase, 1, step])
            )
            blocks(0, step, beside).start()
            part = multiply(at(below, step))
            halves(0, step, beside).wait_recv()
            summed[phase, 1, step, :, half:] = encode(part[:, half:])
            summed[phase, 1, step, :, :half] = encode(
                part[:, :half] + decode(half_theirs[phase, 0, step])
            )
            blocks(1, step, below).start()
        for step in steps:
            total = multiply(at(me, step))
            blocks(0, step, beside).wait_recv()
            total = total + decode(arrived[phase, 0, step])
            blocks(1, step, below).wait_recv()
            total = total + decode(arrived[phase, 1, step])
            if step > 0:
                summed[phase, 2, step] = encode(total)
                blocks(2, step, at(me, step)).start()
        for step in range(1, planes):
            blocks(2, step, at(me, step)).wait_recv()
            total = total + decode(arrived[phase, 2, step])
        for step in steps:
            halves(0, step, beside).wait_send()
            halves(1, step, below).wait_send()
            blocks(0, step, beside).wait_send()
            blocks(1, step, below).wait_send()
            if step > 0:
                blocks(2, step, at(me, step)).wait_send()
        return total

    def project(phase, residual):
        if phase == 0:
            sketch_copy.wait()
        parts = jnp.dot(split(residual), sketch[...], preferred_element_type=jnp.float32)
        total = jnp.concatenate(
            [parts[:strengths] + parts[strengths:], lane_sums(residual * residual)], axis=1
        )
        for step in range(feats):
            proj_mine[phase, step] = total[step * band : (step + 1) * band]

        def swap(step):
            other = lax.rem(side + step, feats)
            return put(
                proj_mine.at[phase, other], proj_theirs.at[phase, step], proj_sems,
                (phase, step), me, other,
            )

        for step in range(1, feats):
            swap(step).start()
        part = proj_mine[phase, side]
        for step in range(1, feats):
            swap(step).wait()
            part = part + proj_theirs[phase, step]

        plane_mine[phase] = part
        corner = me // PLANE * PLANE

        def spread(step):
            return put(
                plane_mine.at[phase], plane_theirs.at[phase, step], plane_sems, (phase, step),
                corner + lax.rem(me - corner + step, PLANE), side,
            )

        for step in range(1, PLANE):
            spread(step).start()
        for step in range(1, PLANE):
            spread(step).wait()
            part = part + plane_theirs[phase, step]

        line_mine[phase] = part

        def along(step):
            return put(
                line_mine.at[phase], line_theirs.at[phase, step], line_sems, (phase, step),
                lax.rem(me + step * PLANE, n), side,
            )

        for step in range(1, planes):
            along(step).start()
        for step in range(1, planes):
            along(step).wait()
            part = part + line_theirs[phase, step]

        proj_full[phase, side] = part

        def back(step):
            return put(
                proj_full.at[phase, side], proj_full.at[phase, side], back_sems, (phase, step),
                me, lax.rem(side + step, feats),
            )

        for step in range(1, feats):
            back(step).start()
        for step in range(1, feats):
            other = lax.rem(side + feats - step, feats)
            put(
                proj_full.at[phase, other], proj_full.at[phase, other], back_sems, (phase, step),
                me, other,
            ).wait_recv()
        for step in range(1, feats):
            back(step).wait_send()
        total = jnp.concatenate([proj_full[phase, step] for step in range(feats)], axis=0)
        return total[:, :rank], jnp.sum(total[:, rank:], axis=1, keepdims=True)

    def precondition(phase, residual):
        projected, norm = project(phase, residual)
        weighted = ratios * projected
        parts = lax.dot_general(
            split(weighted), sketch[...], (((1,), (1,)), ((), ())),
            preferred_element_type=jnp.float32,
        )
        res_dot = norm + jnp.sum(weighted * projected, axis=1, keepdims=True)
        return residual + parts[:strengths] + parts[strengths:], res_dot

    diagonal = (
        lax.broadcasted_iota(jnp.int32, (strengths, LANES), 0)
        == lax.broadcasted_iota(jnp.int32, (strengths, LANES), 1)
    ).astype(jnp.float32)

    def share(phase, values):
        column = jnp.sum(values, axis=1, keepdims=True)
        curve[phase, 0] = jnp.sum(column * diagonal, axis=0, keepdims=True)

        def copy(step):
            return put(
                curve.at[phase, 0], curve.at[phase, step], curve_sems, (phase, step),
                ahead(step), side,
            )

        for step in range(1, n):
            copy(step).start()
        return copy

    def collect(phase, copy):
        for step in range(1, n):
            copy(step).wait()
        total = curve[phase, 0]
        for step in range(1, n):
            total = total + curve[phase, step]
        return jnp.sum(total * diagonal, axis=1, keepdims=True)

    strength = lambdas[...]
    spectrum = sketch_values[...]
    smallest = jnp.min(spectrum, axis=1, keepdims=True)
    ratios = (smallest + strength) / (spectrum + strength) - 1.0

    logits, _ = apply_rows(0)
    probability = jax.nn.sigmoid(logits)
    hessian_diag = probability * (1.0 - probability)
    miss_rows = (probability - labels[...].astype(jnp.float32)).astype(jnp.bfloat16)
    residual = -(apply_columns(0, miss_rows) + strength * weights[...])
    direction, res_dot = precondition(0, residual)
    update = jnp.zeros_like(residual)
    for iteration in range(ITERS):
        gathered[iteration + 1, me] = direction.astype(jnp.bfloat16)
        image, squares = apply_rows(iteration + 1)
        bent = (hessian_diag * image).astype(jnp.bfloat16)
        copy = share(iteration, bent.astype(jnp.float32) * image)
        last = iteration + 1 == ITERS
        if not last:
            hess_dir = apply_columns(iteration + 1, bent) + strength * direction
        curvature = collect(iteration, copy) + strength * squares
        step_size = res_dot / curvature
        update = update + step_size * direction
        if not last:
            residual = residual - step_size * hess_dir
            precond_res, new_dot = precondition(iteration + 1, residual)
            direction = precond_res + (new_dot / res_dot) * direction
            res_dot = new_dot
    out[...] = weights[...] + update


def fused(n, feats, design_matrix, labels, weights, lambdas, sketch, sketch_values):
    strengths, width = weights.shape
    samples = design_matrix.shape[0]
    rank = sketch.shape[1]
    planes = n // PLANE
    band = (strengths // feats, rank + LANES)
    dma = pltpu.SemaphoreType.DMA
    f32, bf16 = jnp.float32, jnp.bfloat16
    vmem = pl.BlockSpec(memory_space=pltpu.VMEM)
    anywhere = pl.BlockSpec(memory_space=pl.ANY)
    return pl.pallas_call(
        functools.partial(kernel, n, feats),
        out_shape=jax.ShapeDtypeStruct(weights.shape, f32),
        in_specs=[anywhere, vmem, vmem, vmem, anywhere, vmem],
        out_specs=vmem,
        scratch_shapes=[
            pltpu.VMEM((n, samples, width), bf16),
            pltpu.VMEM(sketch.shape, bf16),
            pltpu.VMEM((ITERS + 1, n, strengths, width), bf16),
            pltpu.VMEM((ITERS, 2, planes, strengths, width // 2), bf16),
            pltpu.VMEM((ITERS, 2, planes, strengths, width // 2), bf16),
            pltpu.VMEM((ITERS, 3, planes, strengths, width), bf16),
            pltpu.VMEM((ITERS, 3, planes, strengths, width), bf16),
            pltpu.VMEM((ITERS + 1, 2, strengths, samples), f32),
            pltpu.VMEM((ITERS + 1, feats, 2, strengths, samples), f32),
            pltpu.VMEM((ITERS, feats, *band), f32),
            pltpu.VMEM((ITERS, feats, *band), f32),
            pltpu.VMEM((ITERS, feats, *band), f32),
            pltpu.VMEM((ITERS, *band), f32),
            pltpu.VMEM((ITERS, PLANE, *band), f32),
            pltpu.VMEM((ITERS, *band), f32),
            pltpu.VMEM((ITERS, planes, *band), f32),
            pltpu.VMEM((ITERS, n, 1, LANES), f32),
            dma((n,)),
            dma,
            dma((2, ITERS + 1, 5, planes)),
            dma((2, ITERS, 5, planes)),
            dma((2, ITERS + 1, feats)),
            dma((2, ITERS, feats)),
            dma((2, ITERS, PLANE)),
            dma((2, ITERS, planes)),
            dma((2, ITERS, feats)),
            dma((2, ITERS, n)),
        ],
        compiler_params=pltpu.CompilerParams(
            collective_id=0, has_side_effects=True, vmem_limit_bytes=48 * 1024 * 1024
        ),
    )(
        design_matrix, labels[None, :], weights, lambdas[:, None], sketch, sketch_values[None, :]
    )


def solution(mesh):
    n, feats = mesh.shape["samp"], mesh.shape["feat"]

    def local(design_matrix, labels, weights, lambdas, sketch, sketch_values):
        strengths, width = weights.shape
        whole = (
            width % (2 * LANES) == 0
            and design_matrix.shape[0] == LANES
            and sketch.shape[1] % LANES == 0
            and n % PLANE == 0
            and strengths % (8 * feats) == 0
            and strengths <= LANES
        )
        run = functools.partial(fused, n, feats) if whole else shards
        return run(design_matrix, labels, weights, lambdas, sketch, sketch_values)

    return jax.shard_map(
        local,
        mesh=mesh,
        in_specs=(
            P("samp", "feat"),
            P("samp"),
            P(None, ("feat", "samp")),
            P(),
            P(("feat", "samp"), None),
            P(),
        ),
        out_specs=P(None, ("feat", "samp")),
        check_vma=False,
    )
```

```python
import functools

import jax
import jax.numpy as jnp
from jax import lax
from jax.experimental import pallas as pl
from jax.experimental.pallas import tpu as pltpu
from jax.sharding import PartitionSpec as P

ITERS = 2


def shards(design_matrix, labels, weights, lambdas, sketch, sketch_values):
    sketch_full = sketch.astype(jnp.float32)
    smallest = jnp.min(sketch_values)
    ratios = (smallest + lambdas[:, None]) / (sketch_values[None, :] + lambdas[:, None]) - 1.0

    def apply_rows(vector):
        vector_half = vector.astype(jnp.bfloat16)
        partial_rows = lax.dot_general(
            lax.all_gather(vector_half, "samp", axis=1, tiled=True),
            design_matrix,
            (((1,), (1,)), ((), ())),
            preferred_element_type=jnp.float32,
        )
        return lax.psum(partial_rows, "feat")

    def apply_columns(values):
        return lax.psum_scatter(
            lax.dot_general(
                design_matrix, values, (((0,), (1,)), ((), ())), preferred_element_type=jnp.float32
            ),
            "samp",
            scatter_dimension=0,
            tiled=True,
        ).T

    def precondition(residual):
        projected = jnp.dot(residual, sketch_full, precision=lax.Precision.HIGHEST)
        projected = lax.psum(projected, ("samp", "feat"))
        correction = lax.dot_general(
            ratios * projected,
            sketch_full,
            (((1,), (1,)), ((), ())),
            precision=lax.Precision.HIGHEST,
        )
        precond_res = residual + correction
        res_dot = lax.psum(jnp.sum(residual * precond_res, axis=1), ("samp", "feat"))
        return (precond_res, res_dot)

    logits = apply_rows(weights)
    probability = jax.nn.sigmoid(logits)
    hessian_diag = probability * (1.0 - probability)
    miss_rows = (probability - labels[None, :].astype(jnp.float32)).astype(jnp.bfloat16)
    gradient = apply_columns(miss_rows) + lambdas[:, None] * weights
    residual = -gradient
    precond_res, res_dot = precondition(residual)
    direction = precond_res
    update = jnp.zeros_like(residual)
    for iteration in range(ITERS):
        image_rows = apply_rows(direction)
        hess_dir = (
            apply_columns((hessian_diag * image_rows).astype(jnp.bfloat16))
            + lambdas[:, None] * direction
        )
        curvature = lax.psum(jnp.sum(direction * hess_dir, axis=1), ("samp", "feat"))
        step_size = res_dot / curvature
        update = update + step_size[:, None] * direction
        if iteration + 1 < ITERS:
            residual = residual - step_size[:, None] * hess_dir
            precond_res, new_dot = precondition(residual)
            direction = precond_res + (new_dot / res_dot)[:, None] * direction
            res_dot = new_dot
    return weights + update


MESH = pl.DeviceIdType.MESH
LANES = 128
PLANE = 4


def lane_sums(values):
    total = values[:, :LANES]
    for start in range(LANES, values.shape[1], LANES):
        total = total + values[:, start : start + LANES]
    return total


def split(values):
    high = values.astype(jnp.bfloat16)
    low = (values - high.astype(jnp.float32)).astype(jnp.bfloat16)
    return jnp.concatenate([high, low], axis=0)


def kernel(
    n, feats, design_hbm, labels_hbm, weights_hbm, lambdas_hbm, sketch_hbm, values_hbm, out,
    design, labels, weights, lambdas, sketch, sketch_values, gathered, half_mine, half_theirs, summed, arrived, rows_mine, rows_theirs,
    proj_mine, proj_theirs, proj_full, plane_mine, plane_theirs, line_mine, line_theirs,
    curve, design_sem, sketch_sem, small_sems, gather_sems, sum_sems, row_sems, proj_sems,
    plane_sems, line_sems, back_sems, curve_sems,
):
    me = lax.axis_index("samp")
    side = lax.axis_index("feat")
    strengths, width = weights.shape
    rank = sketch.shape[1]
    band = strengths // feats
    planes = n // PLANE

    def fetch(chunk):
        return pltpu.make_async_copy(
            design_hbm.at[:, pl.ds(chunk * width, width)], design.at[chunk], design_sem.at[chunk]
        )

    weights_copy = pltpu.make_async_copy(weights_hbm, weights, small_sems.at[0])
    weights_copy.start()
    small_copies = (
        pltpu.make_async_copy(labels_hbm, labels, small_sems.at[1]),
        pltpu.make_async_copy(lambdas_hbm, lambdas, small_sems.at[2]),
        pltpu.make_async_copy(values_hbm, sketch_values, small_sems.at[3]),
    )
    for copy in small_copies:
        copy.start()
    for chunk in range(n):
        fetch(chunk).start()
    sketch_copy = pltpu.make_async_copy(sketch_hbm, sketch, sketch_sem)
    sketch_copy.start()

    def put(source, target, sems, slot, samp, feat):
        return pltpu.make_async_remote_copy(
            src_ref=source, dst_ref=target,
            send_sem=sems.at[(0, *slot)], recv_sem=sems.at[(1, *slot)],
            device_id=(samp, feat), device_id_type=MESH,
        )

    column = lax.rem(me, 2)
    line = lax.rem(me // 2, 2)
    beside = me + 1 - 2 * column
    below = me + 2 - 4 * line
    across = beside + 2 - 4 * line
    half = width // 2

    level = me // PLANE

    def at(place, step):
        other, bit = 0, 1
        while bit < planes:
            other = other + lax.rem(level // bit + step // bit, 2) * bit
            bit *= 2
        return place + (other - level) * PLANE

    barrier = pltpu.get_barrier_semaphore()
    for partner in (beside, below, across, *(at(me, step) for step in range(1, planes))):
        pl.semaphore_signal(barrier, inc=1, device_id=(partner, side), device_id_type=MESH)
    for step in range(1, feats):
        pl.semaphore_signal(
            barrier, inc=1, device_id=(me, lax.rem(side + step, feats)), device_id_type=MESH
        )
    weights_copy.wait()
    gathered[0, me] = weights[...].astype(jnp.bfloat16)
    pl.semaphore_wait(barrier, PLANE - 1 + planes - 1 + feats - 1)

    def ahead(step):
        return lax.rem(me + step, n)

    def apply_rows(phase):
        copies = []

        def send(chunk, kind, step, target, part=slice(None)):
            block = gathered.at[phase, chunk, :, part]
            copy = put(block, block, gather_sems, (phase, kind, step), target, side)
            copy.start()
            copies.append(copy)

        def receive(chunk, kind, step, part=slice(None)):
            block = gathered.at[phase, chunk, :, part]
            put(block, block, gather_sems, (phase, kind, step), beside, side).wait_recv()

        def multiply(chunk, carry):
            rows, squares = carry
            if phase == 0:
                fetch(chunk).wait()
            block = gathered[phase, chunk]
            rows = rows + lax.dot_general(
                block, design[chunk], (((1,), (1,)), ((), ())), preferred_element_type=jnp.float32
            )
            if phase > 0:
                block = block.astype(jnp.float32)
                squares = squares + lane_sums(block * block)
            return rows, squares

        left, right = slice(0, half), slice(half, width)
        send(me, 0, 0, beside)
        send(me, 1, 0, below)
        for step in range(1, planes):
            send(me, 4, step, at(me, step))
        zero = jnp.zeros((strengths, LANES), jnp.float32)
        carry = (jnp.zeros((strengths, design.shape[1]), jnp.float32), zero)
        carry = multiply(me, carry)
        for step in range(planes):
            if step + 1 < planes:
                chunk = at(me, step + 1)
                receive(chunk, 4, step + 1)
                send(chunk, 0, step + 1, beside)
                send(chunk, 1, step + 1, below)
                carry = multiply(chunk, carry)
            chunk = at(beside, step)
            receive(chunk, 0, step)
            send(chunk, 2, step, below, left)
            other = at(below, step)
            receive(other, 1, step)
            send(other, 3, step, beside, right)
            carry = multiply(chunk, carry)
            carry = multiply(other, carry)
        for step in range(planes):
            chunk = at(across, step)
            receive(chunk, 2, step, left)
            receive(chunk, 3, step, right)
            carry = multiply(chunk, carry)
        rows, squares = carry
        rows_mine[phase, 0] = rows
        rows_mine[phase, 1] = squares

        def swap(step):
            return put(
                rows_mine.at[phase], rows_theirs.at[phase, step], row_sems, (phase, step),
                me, lax.rem(side + step, feats),
            )

        for step in range(1, feats):
            swap(step).start()
        for step in range(1, feats):
            swap(step).wait()
            rows = rows + rows_theirs[phase, step, 0]
            squares = squares + rows_theirs[phase, step, 1]
        for copy in copies:
            copy.wait_send()
        return rows, jnp.sum(squares, axis=1, keepdims=True)

    def encode(values):
        return (values * values * values).astype(jnp.bfloat16)

    def decode(values):
        values = values.astype(jnp.float32)
        root = jnp.exp(jnp.log(jnp.abs(values)) * (1.0 / 3.0))
        return jnp.where(values < 0, -root, root)

    def apply_columns(phase, values):
        def halves(kind, step, target):
            return put(
                half_mine.at[phase, kind, step], half_theirs.at[phase, kind, step], sum_sems,
                (phase, kind, step), target, side,
            )

        def blocks(kind, step, target):
            return put(
                summed.at[phase, kind, step], arrived.at[phase, kind, step], sum_sems,
                (phase, 2 + kind, step), target, side,
            )

        def multiply(chunk):
            return jnp.dot(values, design[chunk], preferred_element_type=jnp.float32)

        steps = tuple(reversed(range(planes)))
        for step in steps:
            part = encode(multiply(at(across, step)))
            half_mine[phase, 0, step] = part[:, :half]
            half_mine[phase, 1, step] = part[:, half:]
            halves(0, step, beside).start()
            halves(1, step, below).start()
        for step in steps:
            part = multiply(at(beside, step))
            halves(1, step, below).wait_recv()
            summed[phase, 0, step, :, :half] = encode(part[:, :half])
            summed[phase, 0, step, :, half:] = encode(
                part[:, half:] + decode(half_theirs[phase, 1, step])
            )
            blocks(0, step, beside).start()
            part = multiply(at(below, step))
            halves(0, step, beside).wait_recv()
            summed[phase, 1, step, :, half:] = encode(part[:, half:])
            summed[phase, 1, step, :, :half] = encode(
                part[:, :half] + decode(half_theirs[phase, 0, step])
            )
            blocks(1, step, below).start()
        for step in steps:
            total = multiply(at(me, step))
            blocks(0, step, beside).wait_recv()
            total = total + decode(arrived[phase, 0, step])
            blocks(1, step, below).wait_recv()
            total = total + decode(arrived[phase, 1, step])
            if step > 0:
                summed[phase, 2, step] = encode(total)
                blocks(2, step, at(me, step)).start()
        for step in range(1, planes):
            blocks(2, step, at(me, step)).wait_recv()
            total = total + decode(arrived[phase, 2, step])
        for step in steps:
            halves(0, step, beside).wait_send()
            halves(1, step, below).wait_send()
            blocks(0, step, beside).wait_send()
            blocks(1, step, below).wait_send()
            if step > 0:
                blocks(2, step, at(me, step)).wait_send()
        return total

    def project(phase, residual):
        if phase == 0:
            sketch_copy.wait()
        parts = jnp.dot(split(residual), sketch[...], preferred_element_type=jnp.float32)
        total = jnp.concatenate(
            [parts[:strengths] + parts[strengths:], lane_sums(residual * residual)], axis=1
        )
        for step in range(feats):
            proj_mine[phase, step] = total[step * band : (step + 1) * band]

        def swap(step):
            other = lax.rem(side + step, feats)
            return put(
                proj_mine.at[phase, other], proj_theirs.at[phase, step], proj_sems,
                (phase, step), me, other,
            )

        for step in range(1, feats):
            swap(step).start()
        part = proj_mine[phase, side]
        for step in range(1, feats):
            swap(step).wait()
            part = part + proj_theirs[phase, step]

        plane_mine[phase] = part
        corner = me // PLANE * PLANE

        def spread(step):
            return put(
                plane_mine.at[phase], plane_theirs.at[phase, step], plane_sems, (phase, step),
                corner + lax.rem(me - corner + step, PLANE), side,
            )

        for step in range(1, PLANE):
            spread(step).start()
        for step in range(1, PLANE):
            spread(step).wait()
            part = part + plane_theirs[phase, step]

        line_mine[phase] = part

        def along(step):
            return put(
                line_mine.at[phase], line_theirs.at[phase, step], line_sems, (phase, step),
                at(me, step), side,
            )

        for step in range(1, planes):
            along(step).start()
        for step in range(1, planes):
            along(step).wait()
            part = part + line_theirs[phase, step]

        proj_full[phase, side] = part

        def back(step):
            return put(
                proj_full.at[phase, side], proj_full.at[phase, side], back_sems, (phase, step),
                me, lax.rem(side + step, feats),
            )

        for step in range(1, feats):
            back(step).start()
        for step in range(1, feats):
            other = lax.rem(side + feats - step, feats)
            put(
                proj_full.at[phase, other], proj_full.at[phase, other], back_sems, (phase, step),
                me, other,
            ).wait_recv()
        for step in range(1, feats):
            back(step).wait_send()
        total = jnp.concatenate([proj_full[phase, step] for step in range(feats)], axis=0)
        return total[:, :rank], jnp.sum(total[:, rank:], axis=1, keepdims=True)

    def precondition(phase, residual):
        projected, norm = project(phase, residual)
        weighted = ratios * projected
        parts = lax.dot_general(
            split(weighted), sketch[...], (((1,), (1,)), ((), ())),
            preferred_element_type=jnp.float32,
        )
        res_dot = norm + jnp.sum(weighted * projected, axis=1, keepdims=True)
        return residual + parts[:strengths] + parts[strengths:], res_dot

    diagonal = (
        lax.broadcasted_iota(jnp.int32, (strengths, LANES), 0)
        == lax.broadcasted_iota(jnp.int32, (strengths, LANES), 1)
    ).astype(jnp.float32)

    def share(phase, values):
        column = jnp.sum(values, axis=1, keepdims=True)
        curve[phase, 0] = jnp.sum(column * diagonal, axis=0, keepdims=True)

        def copy(step):
            return put(
                curve.at[phase, 0], curve.at[phase, step], curve_sems, (phase, step),
                ahead(step), side,
            )

        for step in range(1, n):
            copy(step).start()
        return copy

    def collect(phase, copy):
        for step in range(1, n):
            copy(step).wait()
        total = curve[phase, 0]
        for step in range(1, n):
            total = total + curve[phase, step]
        return jnp.sum(total * diagonal, axis=1, keepdims=True)

    logits, _ = apply_rows(0)
    for copy in small_copies:
        copy.wait()
    strength = jnp.sum(lambdas[...] * diagonal[:, :strengths], axis=1, keepdims=True)
    spectrum = sketch_values[...][None, :]
    smallest = jnp.min(spectrum, axis=1, keepdims=True)
    ratios = (smallest + strength) / (spectrum + strength) - 1.0
    probability = jax.nn.sigmoid(logits)
    hessian_diag = probability * (1.0 - probability)
    miss_rows = (probability - labels[...].astype(jnp.float32)).astype(jnp.bfloat16)
    residual = -(apply_columns(0, miss_rows) + strength * weights[...])
    direction, res_dot = precondition(0, residual)
    update = jnp.zeros_like(residual)
    for iteration in range(ITERS):
        gathered[iteration + 1, me] = direction.astype(jnp.bfloat16)
        image, squares = apply_rows(iteration + 1)
        bent = (hessian_diag * image).astype(jnp.bfloat16)
        copy = share(iteration, bent.astype(jnp.float32) * image)
        last = iteration + 1 == ITERS
        if not last:
            hess_dir = apply_columns(iteration + 1, bent) + strength * direction
        curvature = collect(iteration, copy) + strength * squares
        step_size = res_dot / curvature
        update = update + step_size * direction
        if not last:
            residual = residual - step_size * hess_dir
            precond_res, new_dot = precondition(iteration + 1, residual)
            direction = precond_res + (new_dot / res_dot) * direction
            res_dot = new_dot
    out[...] = weights[...] + update


def fused(n, feats, design_matrix, labels, weights, lambdas, sketch, sketch_values):
    strengths, width = weights.shape
    samples = design_matrix.shape[0]
    rank = sketch.shape[1]
    planes = n // PLANE
    band = (strengths // feats, rank + LANES)
    dma = pltpu.SemaphoreType.DMA
    f32, bf16 = jnp.float32, jnp.bfloat16
    vmem = pl.BlockSpec(memory_space=pltpu.VMEM)
    anywhere = pl.BlockSpec(memory_space=pl.ANY)
    return pl.pallas_call(
        functools.partial(kernel, n, feats),
        out_shape=jax.ShapeDtypeStruct(weights.shape, f32),
        in_specs=[anywhere] * 6,
        out_specs=vmem,
        scratch_shapes=[
            pltpu.VMEM((n, samples, width), bf16),
            pltpu.VMEM((1, samples), jnp.int32),
            pltpu.VMEM(weights.shape, f32),
            pltpu.VMEM((1, strengths), f32),
            pltpu.VMEM(sketch.shape, bf16),
            pltpu.VMEM(sketch_values.shape, f32),
            pltpu.VMEM((ITERS + 1, n, strengths, width), bf16),
            pltpu.VMEM((ITERS, 2, planes, strengths, width // 2), bf16),
            pltpu.VMEM((ITERS, 2, planes, strengths, width // 2), bf16),
            pltpu.VMEM((ITERS, 3, planes, strengths, width), bf16),
            pltpu.VMEM((ITERS, 3, planes, strengths, width), bf16),
            pltpu.VMEM((ITERS + 1, 2, strengths, samples), f32),
            pltpu.VMEM((ITERS + 1, feats, 2, strengths, samples), f32),
            pltpu.VMEM((ITERS, feats, *band), f32),
            pltpu.VMEM((ITERS, feats, *band), f32),
            pltpu.VMEM((ITERS, feats, *band), f32),
            pltpu.VMEM((ITERS, *band), f32),
            pltpu.VMEM((ITERS, PLANE, *band), f32),
            pltpu.VMEM((ITERS, *band), f32),
            pltpu.VMEM((ITERS, planes, *band), f32),
            pltpu.VMEM((ITERS, n, 1, LANES), f32),
            dma((n,)),
            dma,
            dma((4,)),
            dma((2, ITERS + 1, 5, planes)),
            dma((2, ITERS, 5, planes)),
            dma((2, ITERS + 1, feats)),
            dma((2, ITERS, feats)),
            dma((2, ITERS, PLANE)),
            dma((2, ITERS, planes)),
            dma((2, ITERS, feats)),
            dma((2, ITERS, n)),
        ],
        compiler_params=pltpu.CompilerParams(
            collective_id=0, has_side_effects=True, vmem_limit_bytes=63 * 1024 * 1024
        ),
    )(
        design_matrix, labels[None, :], weights, lambdas[None, :], sketch, sketch_values
    )


def solution(mesh):
    n, feats = mesh.shape["samp"], mesh.shape["feat"]

    def local(design_matrix, labels, weights, lambdas, sketch, sketch_values):
        strengths, width = weights.shape
        whole = (
            width % (2 * LANES) == 0
            and design_matrix.shape[0] == LANES
            and sketch.shape[1] % LANES == 0
            and n % PLANE == 0
            and n & (n - 1) == 0
            and strengths % (8 * feats) == 0
            and strengths <= LANES
        )
        run = functools.partial(fused, n, feats) if whole else shards
        return run(design_matrix, labels, weights, lambdas, sketch, sketch_values)

    return jax.shard_map(
        local,
        mesh=mesh,
        in_specs=(
            P("samp", "feat"),
            P("samp"),
            P(None, ("feat", "samp")),
            P(),
            P(("feat", "samp"), None),
            P(),
        ),
        out_specs=P(None, ("feat", "samp")),
        check_vma=False,
    )
```

```python
import functools

import jax
import jax.numpy as jnp
from jax import lax
from jax.experimental import pallas as pl
from jax.experimental.pallas import tpu as pltpu
from jax.sharding import PartitionSpec as P

ITERS = 2


def shards(design_matrix, labels, weights, lambdas, sketch, sketch_values):
    sketch_full = sketch.astype(jnp.float32)
    smallest = jnp.min(sketch_values)
    ratios = (smallest + lambdas[:, None]) / (sketch_values[None, :] + lambdas[:, None]) - 1.0

    def apply_rows(vector):
        vector_half = vector.astype(jnp.bfloat16)
        partial_rows = lax.dot_general(
            lax.all_gather(vector_half, "samp", axis=1, tiled=True),
            design_matrix,
            (((1,), (1,)), ((), ())),
            preferred_element_type=jnp.float32,
        )
        return lax.psum(partial_rows, "feat")

    def apply_columns(values):
        return lax.psum_scatter(
            lax.dot_general(
                design_matrix, values, (((0,), (1,)), ((), ())), preferred_element_type=jnp.float32
            ),
            "samp",
            scatter_dimension=0,
            tiled=True,
        ).T

    def precondition(residual):
        projected = jnp.dot(residual, sketch_full, precision=lax.Precision.HIGHEST)
        projected = lax.psum(projected, ("samp", "feat"))
        correction = lax.dot_general(
            ratios * projected,
            sketch_full,
            (((1,), (1,)), ((), ())),
            precision=lax.Precision.HIGHEST,
        )
        precond_res = residual + correction
        res_dot = lax.psum(jnp.sum(residual * precond_res, axis=1), ("samp", "feat"))
        return (precond_res, res_dot)

    logits = apply_rows(weights)
    probability = jax.nn.sigmoid(logits)
    hessian_diag = probability * (1.0 - probability)
    miss_rows = (probability - labels[None, :].astype(jnp.float32)).astype(jnp.bfloat16)
    gradient = apply_columns(miss_rows) + lambdas[:, None] * weights
    residual = -gradient
    precond_res, res_dot = precondition(residual)
    direction = precond_res
    update = jnp.zeros_like(residual)
    for iteration in range(ITERS):
        image_rows = apply_rows(direction)
        hess_dir = (
            apply_columns((hessian_diag * image_rows).astype(jnp.bfloat16))
            + lambdas[:, None] * direction
        )
        curvature = lax.psum(jnp.sum(direction * hess_dir, axis=1), ("samp", "feat"))
        step_size = res_dot / curvature
        update = update + step_size[:, None] * direction
        if iteration + 1 < ITERS:
            residual = residual - step_size[:, None] * hess_dir
            precond_res, new_dot = precondition(residual)
            direction = precond_res + (new_dot / res_dot)[:, None] * direction
            res_dot = new_dot
    return weights + update


MESH = pl.DeviceIdType.MESH
LANES = 128
PLANE = 4


def lane_sums(values):
    total = values[:, :LANES]
    for start in range(LANES, values.shape[1], LANES):
        total = total + values[:, start : start + LANES]
    return total


def split(values):
    high = values.astype(jnp.bfloat16)
    low = (values - high.astype(jnp.float32)).astype(jnp.bfloat16)
    return jnp.concatenate([high, low], axis=0)


def kernel(
    n, feats, design_hbm, labels_hbm, weights_hbm, lambdas_hbm, sketch_hbm, values_hbm, out,
    design, labels, weights, lambdas, sketch, sketch_values, gathered, half_mine, half_theirs, summed, arrived, rows_mine, rows_theirs,
    proj_mine, proj_theirs, proj_full, plane_mine, plane_theirs, line_mine, line_theirs,
    curve, design_sem, sketch_sem, small_sems, gather_sems, sum_sems, row_sems, proj_sems,
    plane_sems, line_sems, back_sems, curve_sems,
):
    me = lax.axis_index("samp")
    side = lax.axis_index("feat")
    strengths, width = weights.shape
    rank = sketch.shape[1]
    band = strengths // feats
    planes = n // PLANE

    def fetch(chunk):
        return pltpu.make_async_copy(
            design_hbm.at[:, pl.ds(chunk * width, width)], design.at[chunk], design_sem.at[chunk]
        )

    weights_copy = pltpu.make_async_copy(weights_hbm, weights, small_sems.at[0])
    weights_copy.start()
    small_copies = (
        pltpu.make_async_copy(labels_hbm, labels, small_sems.at[1]),
        pltpu.make_async_copy(lambdas_hbm, lambdas, small_sems.at[2]),
        pltpu.make_async_copy(values_hbm, sketch_values, small_sems.at[3]),
    )
    for copy in small_copies:
        copy.start()
    for chunk in range(n):
        fetch(chunk).start()
    sketch_copy = pltpu.make_async_copy(sketch_hbm, sketch, sketch_sem)
    sketch_copy.start()

    def put(source, target, sems, slot, samp, feat):
        return pltpu.make_async_remote_copy(
            src_ref=source, dst_ref=target,
            send_sem=sems.at[(0, *slot)], recv_sem=sems.at[(1, *slot)],
            device_id=(samp, feat), device_id_type=MESH,
        )

    column = lax.rem(me, 2)
    line = lax.rem(me // 2, 2)
    beside = me + 1 - 2 * column
    below = me + 2 - 4 * line
    across = beside + 2 - 4 * line
    half = width // 2
    far = planes - 1

    level = me // PLANE

    def at(place, step):
        other, bit = 0, 1
        while bit < planes:
            other = other + lax.rem(level // bit + step // bit, 2) * bit
            bit *= 2
        return place + (other - level) * PLANE

    barrier = pltpu.get_barrier_semaphore()
    for partner in (beside, below, across, *(at(me, step) for step in range(1, planes))):
        pl.semaphore_signal(barrier, inc=1, device_id=(partner, side), device_id_type=MESH)
    for step in range(1, feats):
        pl.semaphore_signal(
            barrier, inc=1, device_id=(me, lax.rem(side + step, feats)), device_id_type=MESH
        )
    weights_copy.wait()
    gathered[0, me] = weights[...].astype(jnp.bfloat16)
    pl.semaphore_wait(barrier, PLANE - 1 + planes - 1 + feats - 1)

    def ahead(step):
        return lax.rem(me + step, n)

    def apply_rows(phase):
        copies = []

        def send(chunk, kind, step, target, part=slice(None)):
            block = gathered.at[phase, chunk, :, part]
            copy = put(block, block, gather_sems, (phase, kind, step), target, side)
            copy.start()
            copies.append(copy)

        def receive(chunk, kind, step, part=slice(None)):
            block = gathered.at[phase, chunk, :, part]
            put(block, block, gather_sems, (phase, kind, step), beside, side).wait_recv()

        def multiply(chunk, carry):
            rows, squares = carry
            if phase == 0:
                fetch(chunk).wait()
            block = gathered[phase, chunk]
            rows = rows + lax.dot_general(
                block, design[chunk], (((1,), (1,)), ((), ())), preferred_element_type=jnp.float32
            )
            if phase > 0:
                block = block.astype(jnp.float32)
                squares = squares + lane_sums(block * block)
            return rows, squares

        left, right = slice(0, half), slice(half, width)
        send(me, 0, 0, beside)
        send(me, 1, 0, below)
        for step in range(1, planes):
            send(me, 4, step, at(me, step))
        send(me, 2, 0, across)
        zero = jnp.zeros((strengths, LANES), jnp.float32)
        carry = (jnp.zeros((strengths, design.shape[1]), jnp.float32), zero)
        carry = multiply(me, carry)
        for step in range(planes):
            if step + 1 < planes:
                chunk = at(me, step + 1)
                receive(chunk, 4, step + 1)
                send(chunk, 0, step + 1, beside)
                send(chunk, 1, step + 1, below)
                carry = multiply(chunk, carry)
            relayed = 0 < step < far
            chunk = at(beside, step)
            receive(chunk, 0, step)
            if relayed:
                send(chunk, 2, step, below, left)
            other = at(below, step)
            receive(other, 1, step)
            if relayed:
                send(other, 3, step, beside, right)
            carry = multiply(chunk, carry)
            carry = multiply(other, carry)
            if step == 0:
                receive(across, 2, 0)
                send(across, 4, 0, at(me, far))
                carry = multiply(across, carry)
        for step in range(1, far):
            chunk = at(across, step)
            receive(chunk, 2, step, left)
            receive(chunk, 3, step, right)
            carry = multiply(chunk, carry)
        chunk = at(across, far)
        receive(chunk, 4, 0)
        carry = multiply(chunk, carry)
        rows, squares = carry
        rows_mine[phase, 0] = rows
        rows_mine[phase, 1] = squares

        def swap(step):
            return put(
                rows_mine.at[phase], rows_theirs.at[phase, step], row_sems, (phase, step),
                me, lax.rem(side + step, feats),
            )

        for step in range(1, feats):
            swap(step).start()
        for step in range(1, feats):
            swap(step).wait()
            rows = rows + rows_theirs[phase, step, 0]
            squares = squares + rows_theirs[phase, step, 1]
        for copy in copies:
            copy.wait_send()
        return rows, jnp.sum(squares, axis=1, keepdims=True)

    def encode(values):
        return (values * values * values).astype(jnp.bfloat16)

    def decode(values):
        values = values.astype(jnp.float32)
        root = jnp.exp(jnp.log(jnp.abs(values)) * (1.0 / 3.0))
        return jnp.where(values < 0, -root, root)

    def apply_columns(phase, values):
        def halves(kind, step, target):
            return put(
                half_mine.at[phase, kind, step], half_theirs.at[phase, kind, step], sum_sems,
                (phase, kind, step), target, side,
            )

        def blocks(kind, step, target):
            return put(
                summed.at[phase, kind, step], arrived.at[phase, kind, step], sum_sems,
                (phase, 2 + kind, step), target, side,
            )

        def multiply(chunk):
            return jnp.dot(values, design[chunk], preferred_element_type=jnp.float32)

        steps = tuple(reversed(range(planes)))
        middle = steps[1:-1]
        summed[phase, 3, far] = encode(multiply(at(across, far)))
        blocks(3, far, at(me, far)).start()
        for step in middle:
            part = encode(multiply(at(across, step)))
            half_mine[phase, 0, step] = part[:, :half]
            half_mine[phase, 1, step] = part[:, half:]
            halves(0, step, beside).start()
            halves(1, step, below).start()
        for step in steps:
            aside = multiply(at(beside, step))
            under = multiply(at(below, step))
            if step in middle:
                halves(1, step, below).wait_recv()
                more = decode(half_theirs[phase, 1, step])
                aside = jnp.concatenate([aside[:, :half], aside[:, half:] + more], axis=1)
            summed[phase, 0, step] = encode(aside)
            blocks(0, step, beside).start()
            if step in middle:
                halves(0, step, beside).wait_recv()
                more = decode(half_theirs[phase, 0, step])
                under = jnp.concatenate([under[:, :half] + more, under[:, half:]], axis=1)
            summed[phase, 1, step] = encode(under)
            blocks(1, step, below).start()
        for step in steps:
            total = multiply(at(me, step))
            blocks(0, step, beside).wait_recv()
            total = total + decode(arrived[phase, 0, step])
            blocks(1, step, below).wait_recv()
            total = total + decode(arrived[phase, 1, step])
            if step > 0:
                summed[phase, 2, step] = encode(total)
                blocks(2, step, at(me, step)).start()
            if step == far:
                part = multiply(across)
                blocks(3, far, at(me, far)).wait_recv()
                summed[phase, 3, 0] = encode(part + decode(arrived[phase, 3, far]))
                blocks(3, 0, across).start()
        for step in range(1, planes):
            blocks(2, step, at(me, step)).wait_recv()
            total = total + decode(arrived[phase, 2, step])
        blocks(3, 0, across).wait_recv()
        total = total + decode(arrived[phase, 3, 0])
        for step in steps:
            if step in middle:
                halves(0, step, beside).wait_send()
                halves(1, step, below).wait_send()
            blocks(0, step, beside).wait_send()
            blocks(1, step, below).wait_send()
            if step > 0:
                blocks(2, step, at(me, step)).wait_send()
        blocks(3, far, at(me, far)).wait_send()
        blocks(3, 0, across).wait_send()
        return total

    def project(phase, residual):
        if phase == 0:
            sketch_copy.wait()
        parts = jnp.dot(split(residual), sketch[...], preferred_element_type=jnp.float32)
        total = jnp.concatenate(
            [parts[:strengths] + parts[strengths:], lane_sums(residual * residual)], axis=1
        )
        for step in range(feats):
            proj_mine[phase, step] = total[step * band : (step + 1) * band]

        def swap(step):
            other = lax.rem(side + step, feats)
            return put(
                proj_mine.at[phase, other], proj_theirs.at[phase, step], proj_sems,
                (phase, step), me, other,
            )

        for step in range(1, feats):
            swap(step).start()
        part = proj_mine[phase, side]
        for step in range(1, feats):
            swap(step).wait()
            part = part + proj_theirs[phase, step]

        plane_mine[phase] = part.astype(jnp.bfloat16)
        part = plane_mine[phase].astype(jnp.float32)
        corner = me // PLANE * PLANE

        def spread(step):
            return put(
                plane_mine.at[phase], plane_theirs.at[phase, step], plane_sems, (phase, step),
                corner + lax.rem(me - corner + step, PLANE), side,
            )

        for step in range(1, PLANE):
            spread(step).start()
        for step in range(1, PLANE):
            spread(step).wait()
            part = part + plane_theirs[phase, step].astype(jnp.float32)

        line_mine[phase] = part.astype(jnp.bfloat16)
        part = line_mine[phase].astype(jnp.float32)

        def along(step):
            return put(
                line_mine.at[phase], line_theirs.at[phase, step], line_sems, (phase, step),
                at(me, step), side,
            )

        for step in range(1, planes):
            along(step).start()
        for step in range(1, planes):
            along(step).wait()
            part = part + line_theirs[phase, step].astype(jnp.float32)

        proj_full[phase, side] = part

        def back(step):
            return put(
                proj_full.at[phase, side], proj_full.at[phase, side], back_sems, (phase, step),
                me, lax.rem(side + step, feats),
            )

        for step in range(1, feats):
            back(step).start()
        for step in range(1, feats):
            other = lax.rem(side + feats - step, feats)
            put(
                proj_full.at[phase, other], proj_full.at[phase, other], back_sems, (phase, step),
                me, other,
            ).wait_recv()
        for step in range(1, feats):
            back(step).wait_send()
        total = jnp.concatenate([proj_full[phase, step] for step in range(feats)], axis=0)
        return total[:, :rank], jnp.sum(total[:, rank:], axis=1, keepdims=True)

    def precondition(phase, residual):
        projected, norm = project(phase, residual)
        weighted = ratios * projected
        parts = lax.dot_general(
            split(weighted), sketch[...], (((1,), (1,)), ((), ())),
            preferred_element_type=jnp.float32,
        )
        res_dot = norm + jnp.sum(weighted * projected, axis=1, keepdims=True)
        return residual + parts[:strengths] + parts[strengths:], res_dot

    diagonal = (
        lax.broadcasted_iota(jnp.int32, (strengths, LANES), 0)
        == lax.broadcasted_iota(jnp.int32, (strengths, LANES), 1)
    ).astype(jnp.float32)

    def share(phase, values):
        column = jnp.sum(values, axis=1, keepdims=True)
        curve[phase, 0] = jnp.sum(column * diagonal, axis=0, keepdims=True)

        def copy(step):
            return put(
                curve.at[phase, 0], curve.at[phase, step], curve_sems, (phase, step),
                ahead(step), side,
            )

        for step in range(1, n):
            copy(step).start()
        return copy

    def collect(phase, copy):
        for step in range(1, n):
            copy(step).wait()
        total = curve[phase, 0]
        for step in range(1, n):
            total = total + curve[phase, step]
        return jnp.sum(total * diagonal, axis=1, keepdims=True)

    logits, _ = apply_rows(0)
    for copy in small_copies:
        copy.wait()
    strength = jnp.sum(lambdas[...] * diagonal[:, :strengths], axis=1, keepdims=True)
    spectrum = sketch_values[...][None, :]
    smallest = jnp.min(spectrum, axis=1, keepdims=True)
    ratios = (smallest + strength) / (spectrum + strength) - 1.0
    probability = jax.nn.sigmoid(logits)
    hessian_diag = probability * (1.0 - probability)
    miss_rows = (probability - labels[...].astype(jnp.float32)).astype(jnp.bfloat16)
    residual = -(apply_columns(0, miss_rows) + strength * weights[...])
    direction, res_dot = precondition(0, residual)
    update = jnp.zeros_like(residual)
    for iteration in range(ITERS):
        gathered[iteration + 1, me] = direction.astype(jnp.bfloat16)
        image, squares = apply_rows(iteration + 1)
        bent = (hessian_diag * image).astype(jnp.bfloat16)
        copy = share(iteration, bent.astype(jnp.float32) * image)
        last = iteration + 1 == ITERS
        if not last:
            hess_dir = apply_columns(iteration + 1, bent) + strength * direction
        curvature = collect(iteration, copy) + strength * squares
        step_size = res_dot / curvature
        update = update + step_size * direction
        if not last:
            residual = residual - step_size * hess_dir
            precond_res, new_dot = precondition(iteration + 1, residual)
            direction = precond_res + (new_dot / res_dot) * direction
            res_dot = new_dot
    out[...] = weights[...] + update


def fused(n, feats, design_matrix, labels, weights, lambdas, sketch, sketch_values):
    strengths, width = weights.shape
    samples = design_matrix.shape[0]
    rank = sketch.shape[1]
    planes = n // PLANE
    band = (strengths // feats, rank + LANES)
    dma = pltpu.SemaphoreType.DMA
    f32, bf16 = jnp.float32, jnp.bfloat16
    vmem = pl.BlockSpec(memory_space=pltpu.VMEM)
    anywhere = pl.BlockSpec(memory_space=pl.ANY)
    return pl.pallas_call(
        functools.partial(kernel, n, feats),
        out_shape=jax.ShapeDtypeStruct(weights.shape, f32),
        in_specs=[anywhere] * 6,
        out_specs=vmem,
        scratch_shapes=[
            pltpu.VMEM((n, samples, width), bf16),
            pltpu.VMEM((1, samples), jnp.int32),
            pltpu.VMEM(weights.shape, f32),
            pltpu.VMEM((1, strengths), f32),
            pltpu.VMEM(sketch.shape, bf16),
            pltpu.VMEM(sketch_values.shape, f32),
            pltpu.VMEM((ITERS + 1, n, strengths, width), bf16),
            pltpu.VMEM((ITERS, 2, planes, strengths, width // 2), bf16),
            pltpu.VMEM((ITERS, 2, planes, strengths, width // 2), bf16),
            pltpu.VMEM((ITERS, 4, planes, strengths, width), bf16),
            pltpu.VMEM((ITERS, 4, planes, strengths, width), bf16),
            pltpu.VMEM((ITERS + 1, 2, strengths, samples), f32),
            pltpu.VMEM((ITERS + 1, feats, 2, strengths, samples), f32),
            pltpu.VMEM((ITERS, feats, *band), f32),
            pltpu.VMEM((ITERS, feats, *band), f32),
            pltpu.VMEM((ITERS, feats, *band), f32),
            pltpu.VMEM((ITERS, *band), bf16),
            pltpu.VMEM((ITERS, PLANE, *band), bf16),
            pltpu.VMEM((ITERS, *band), bf16),
            pltpu.VMEM((ITERS, planes, *band), bf16),
            pltpu.VMEM((ITERS, n, 1, LANES), f32),
            dma((n,)),
            dma,
            dma((4,)),
            dma((2, ITERS + 1, 5, planes)),
            dma((2, ITERS, 6, planes)),
            dma((2, ITERS + 1, feats)),
            dma((2, ITERS, feats)),
            dma((2, ITERS, PLANE)),
            dma((2, ITERS, planes)),
            dma((2, ITERS, feats)),
            dma((2, ITERS, n)),
        ],
        compiler_params=pltpu.CompilerParams(
            collective_id=0, has_side_effects=True, vmem_limit_bytes=63 * 1024 * 1024
        ),
    )(
        design_matrix, labels[None, :], weights, lambdas[None, :], sketch, sketch_values
    )


def solution(mesh):
    n, feats = mesh.shape["samp"], mesh.shape["feat"]

    def local(design_matrix, labels, weights, lambdas, sketch, sketch_values):
        strengths, width = weights.shape
        whole = (
            width % (2 * LANES) == 0
            and design_matrix.shape[0] == LANES
            and sketch.shape[1] % LANES == 0
            and n % PLANE == 0
            and n > PLANE
            and n & (n - 1) == 0
            and strengths % (8 * feats) == 0
            and strengths <= LANES
        )
        run = functools.partial(fused, n, feats) if whole else shards
        return run(design_matrix, labels, weights, lambdas, sketch, sketch_values)

    return jax.shard_map(
        local,
        mesh=mesh,
        in_specs=(
            P("samp", "feat"),
            P("samp"),
            P(None, ("feat", "samp")),
            P(),
            P(("feat", "samp"), None),
            P(),
        ),
        out_specs=P(None, ("feat", "samp")),
        check_vma=False,
    )
```
